32 devices in a mesh: row: 8 (over y, x, core), col: 4 (over z).
Axes of the slice: x: 2, y: 2, z: 4, core: 2. Of those that a mesh axis runs over, the one named last changes fastest.
Arguments:
- inputs: bfloat16 [1280, 24576], P('col', 'row'), may hold values from -6 to 6
- cotangent: bfloat16 [1280, 24576], P('col', 'row'), may hold values from -6 to 6
- clip_lengths: int32 [16], P('row'), may hold values from 384 to 1536, as said below
- project_weight: float32 [3, 1280, 1280], P(None, 'row', 'col'), may hold values from -0.15625 to 0.15625
- project_moment: float32 [3, 1280, 1280], P(None, 'row', 'col'), may hold values from -80 to 80
- project_average: float32 [3, 1280, 1280], P(None, 'row', 'col'), may hold values from -0.15625 to 0.15625
- output_weight: float32 [1280, 1280], P('col', 'row'), may hold values from -1.25 to 1.25
- output_moment: float32 [1280, 1280], P('col', 'row'), may hold values from -32 to 32
- output_average: float32 [1280, 1280], P('col', 'row'), may hold values from -1.25 to 1.25
- expand_weight: float32 [1280, 5120], P('row', 'col'), may hold values from -0.15625 to 0.15625
- expand_moment: float32 [1280, 5120], P('row', 'col'), may hold values from -224 to 224
- expand_average: float32 [1280, 5120], P('row', 'col'), may hold values from -0.15625 to 0.15625
- reduce_weight: float32 [5120, 1280], P('col', 'row'), may hold values from -0.078125 to 0.078125
- reduce_moment: float32 [5120, 1280], P('col', 'row'), may hold values from -448 to 448
- reduce_average: float32 [5120, 1280], P('col', 'row'), may hold values from -0.078125 to 0.078125
- gain_first: float32 [1280], P('col'), may hold values from 0.1 to 1.9
- first_moment: float32 [1280], P('col'), may hold values from -448 to 448
- first_average: float32 [1280], P('col'), may hold values from 0.1 to 1.9
- gain_second: float32 [1280], P('col'), may hold values from 0.1 to 1.9
- second_moment: float32 [1280], P('col'), may hold values from -448 to 448
- second_average: float32 [1280], P('col'), may hold values from 0.1 to 1.9
Outputs:
- block_output: bfloat16 [1280, 24576], P('col', 'row')
- input_grad: float32 [1280, 24576], P('col', 'row')
- project_grad: float32 [3, 1280, 1280], P(None, 'row', 'col')
- project_moment_next: float32 [3, 1280, 1280], P(None, 'row', 'col')
- project_weight_next: float32 [3, 1280, 1280], P(None, 'row', 'col')
- project_average_next: float32 [3, 1280, 1280], P(None, 'row', 'col')
- project_weight_copy: bfloat16 [3, 1280, 1280], P(None, 'row', 'col')
- output_grad: float32 [1280, 1280], P('col', 'row')
- output_moment_next: float32 [1280, 1280], P('col', 'row')
- output_weight_next: float32 [1280, 1280], P('col', 'row')
- output_average_next: float32 [1280, 1280], P('col', 'row')
- output_weight_copy: bfloat16 [1280, 1280], P('col', 'row')
- expand_grad: float32 [1280, 5120], P('row', 'col')
- expand_moment_next: float32 [1280, 5120], P('row', 'col')
- expand_weight_next: float32 [1280, 5120], P('row', 'col')
- expand_average_next: float32 [1280, 5120], P('row', 'col')
- expand_weight_copy: bfloat16 [1280, 5120], P('row', 'col')
- reduce_grad: float32 [5120, 1280], P('col', 'row')
- reduce_moment_next: float32 [5120, 1280], P('col', 'row')
- reduce_weight_next: float32 [5120, 1280], P('col', 'row')
- reduce_average_next: float32 [5120, 1280], P('col', 'row')
- reduce_weight_copy: bfloat16 [5120, 1280], P('col', 'row')
- gain_first_grad: float32 [1280], P('col')
- first_moment_next: float32 [1280], P('col')
- gain_first_next: float32 [1280], P('col')
- first_average_next: float32 [1280], P('col')
- gain_second_grad: float32 [1280], P('col')
- second_moment_next: float32 [1280], P('col')
- gain_second_next: float32 [1280], P('col')
- second_average_next: float32 [1280], P('col')
The draws below stay inside these ranges and needn't reach their ends.
Inputs may be any that keep to these rules, and one draw needn't show every extreme that they name: `clip_lengths`: real tokens of each clip; the rest of its 1536 slots is padding. Some clip is full and some holds a quarter of 1536.
All inputs are finite; a program needn't handle non-finite values.
Results may differ from the reference program's by a relative error of at most 0.02.
Values may be sent and summed in bfloat16 or wider, within the bound.
A program may use at most 256 MiB of HBM per device.

```python
import math
import jax
import jax.numpy as jnp
from jax import lax

D = 1280
HEADS = 16
HEAD_DIM = 80
FF = 5120
SEQ = 1536
CLIPS = 16
TOKENS = 24576


def draw_clip_lengths(key, part):
    spread_key = jax.random.fold_in(key, 11)
    place_key = jax.random.fold_in(key, 23)
    lengths = jax.random.randint(spread_key, (CLIPS,), SEQ // 4, SEQ + 1)
    places = jax.random.permutation(place_key, CLIPS)
    lengths = lengths.at[places[0]].set(SEQ)
    lengths = lengths.at[places[1]].set(SEQ // 4)
    return lengths.astype(jnp.int32)


def level_of(rng, dims, split, smallest, high):
    loudness, own = 1.0, jax.random.fold_in(rng, 6)
    for axis_at, shards_of in split:
        steps = jnp.exp(jax.random.uniform(jax.random.fold_in(own, axis_at), (shards_of,), jnp.float32, smallest / len(split), high / len(split)))
        loudness = loudness * jnp.repeat(steps, dims[axis_at] // shards_of).reshape([-1 if axis == axis_at else 1 for axis in range(len(dims))])
    return loudness


def scatter_about(key, shape, scale, limit, shards=(), held_as=jnp.bfloat16):
    level = level_of(key, shape, shards, -0.22, 0.18) if shards else 1.0
    drawn = jax.random.normal(key, shape, jnp.float32) * scale * level
    return jnp.minimum(jnp.maximum(drawn, -limit), limit).astype(held_as)


def setup_inputs(seed: int = 0) -> dict:
    keys = jax.random.split(jax.random.key(seed), 22)
    return {
        "inputs": scatter_about(keys[0], (D, TOKENS), 1.0, 6.0, ((0, 4), (1, 8))),
        "cotangent": scatter_about(keys[1], (D, TOKENS), 1.0, 6.0, ((0, 4), (1, 8))),
        "clip_lengths": draw_clip_lengths(jax.random.fold_in(keys[21], 71), 0),
        "project_weight": scatter_about(keys[3], (3, D, D), D ** -0.5, 0.15625, ((1, 8), (2, 4)), jnp.float32),
        "project_moment": scatter_about(keys[4], (3, D, D), (0.08 * TOKENS ** 0.5), 80.0, ((1, 8), (2, 4)), jnp.float32),
        "project_average": scatter_about(keys[5], (3, D, D), D ** -0.5, 0.15625, ((1, 8), (2, 4)), jnp.float32),
        "output_weight": scatter_about(keys[6], (D, D), (D // 64) ** -0.5, 1.25, ((0, 4), (1, 8)), jnp.float32),
        "output_moment": scatter_about(keys[7], (D, D), (0.035 * TOKENS ** 0.5), 32.0, ((0, 4), (1, 8)), jnp.float32),
        "output_average": scatter_about(keys[8], (D, D), (D // 64) ** -0.5, 1.25, ((0, 4), (1, 8)), jnp.float32),
        "expand_weight": scatter_about(keys[9], (D, FF), D ** -0.5, 0.15625, ((0, 8), (1, 4)), jnp.float32),
        "expand_moment": scatter_about(keys[10], (D, FF), (0.25 * TOKENS ** 0.5), 224.0, ((0, 8), (1, 4)), jnp.float32),
        "expand_average": scatter_about(keys[11], (D, FF), D ** -0.5, 0.15625, ((0, 8), (1, 4)), jnp.float32),
        "reduce_weight": scatter_about(keys[12], (FF, D), FF ** -0.5, 0.078125, ((0, 4), (1, 8)), jnp.float32),
        "reduce_moment": scatter_about(keys[13], (FF, D), (0.5 * TOKENS ** 0.5), 448.0, ((0, 4), (1, 8)), jnp.float32),
        "reduce_average": scatter_about(keys[14], (FF, D), FF ** -0.5, 0.078125, ((0, 4), (1, 8)), jnp.float32),
        "gain_first": jnp.clip(1.0 + 0.18 * jax.random.normal(keys[15], (D,), jnp.float32), 0.1, 1.9),
        "first_moment": scatter_about(keys[16], (D,), (0.5 * TOKENS ** 0.5), 448.0, ((0, 4),), jnp.float32),
        "first_average": jnp.clip(1.0 + 0.18 * jax.random.normal(keys[17], (D,), jnp.float32), 0.1, 1.9),
        "gain_second": jnp.clip(1.0 + 0.18 * jax.random.normal(keys[18], (D,), jnp.float32), 0.1, 1.9),
        "second_moment": scatter_about(keys[19], (D,), (0.5 * TOKENS ** 0.5), 448.0, ((0, 4),), jnp.float32),
        "second_average": jnp.clip(1.0 + 0.18 * jax.random.normal(keys[20], (D,), jnp.float32), 0.1, 1.9),
    }


EPS = 1e-05
NEG = -1e+30
MOMENTUM = 0.9
AVERAGING = 0.6
RATE_PROJECT = 0.07
RATE_OUTPUT = 3.5
RATE_EXPAND = 0.06
RATE_REDUCE = 0.015
RATE_GAIN = 0.2

@jax.custom_vjp
def low(v):
    return lax.optimization_barrier(v.astype(jnp.bfloat16)).astype(jnp.float32)

@jax.custom_vjp
def low_back(v):
    return v

def low_keep(v):
    return (low(v), None)

def low_pass(kept, grad):
    return (grad,)

def back_keep(v):
    return (v, None)

def back_low(kept, grad):
    return (low(grad),)
low.defvjp(low_keep, low_pass)
low_back.defvjp(back_keep, back_low)

def layer_norm(values, gain):
    average = lax.optimization_barrier(jnp.mean(values, axis=-1, keepdims=True))
    spread = lax.optimization_barrier(jnp.mean(values * values, axis=-1, keepdims=True)) - average * average
    return (values - average) * lax.rsqrt(spread + EPS) * gain

def clip_attention(operands):
    query_rows, key_rows, value_rows, length = operands
    scores = jnp.einsum('qhd,khd->hqk', query_rows, key_rows, precision=lax.Precision.HIGHEST) * (1.0 / math.sqrt(HEAD_DIM))
    scores = low_back(scores)
    keys_ok = jnp.arange(SEQ, dtype=jnp.int32) < length
    scores = jnp.where(keys_ok[None, None, :], scores, NEG)
    highest = lax.optimization_barrier(jnp.max(scores, axis=-1, keepdims=True))
    powers = jnp.exp(scores - highest)
    probs = low(powers / lax.optimization_barrier(jnp.sum(powers, axis=-1, keepdims=True)))
    return jnp.einsum('hqk,khd->qhd', probs, value_rows, precision=lax.Precision.HIGHEST)

def forward(resident, project_w, output_w, expand_w, reduce_w, gain_one, gain_two, clip_lengths):
    hidden_one = low(layer_norm(resident, gain_one))
    projected = jnp.einsum('td,kde->kte', hidden_one, low(project_w), precision=lax.Precision.HIGHEST)
    projected = low(low_back(projected))
    split_rows = projected.reshape(3, CLIPS, SEQ, HEADS, HEAD_DIM)
    attended = lax.map(jax.checkpoint(clip_attention), (split_rows[0], split_rows[1], split_rows[2], clip_lengths))
    attended = low(low_back(attended.reshape(TOKENS, D)))
    branch = low_back(jnp.dot(attended, low(output_w), precision=lax.Precision.HIGHEST, preferred_element_type=jnp.float32))
    middle = resident + branch
    hidden_two = low(layer_norm(middle, gain_two))
    pre_act = low_back(jnp.dot(hidden_two, low(expand_w), precision=lax.Precision.HIGHEST, preferred_element_type=jnp.float32))
    activated = low(jax.nn.gelu(pre_act, approximate=False))
    mlp_out = low_back(jnp.dot(activated, low(reduce_w), precision=lax.Precision.HIGHEST, preferred_element_type=jnp.float32))
    return middle + mlp_out

def update(weight, moment, average, gradient, rate):
    moment_next = MOMENTUM * moment + gradient
    weight_next = weight - rate * (gradient + MOMENTUM * moment_next)
    average_next = AVERAGING * average + (1.0 - AVERAGING) * weight_next
    return (moment_next, weight_next, average_next)

def reference(inputs, cotangent, clip_lengths, project_weight, project_moment, project_average, output_weight, output_moment, output_average, expand_weight, expand_moment, expand_average, reduce_weight, reduce_moment, reduce_average, gain_first, first_moment, first_average, gain_second, second_moment, second_average):
    resident = inputs.astype(jnp.float32).T
    positions = jnp.arange(SEQ, dtype=jnp.int32)
    row_mask = (positions[None, :] < clip_lengths[:, None]).astype(jnp.float32).reshape(TOKENS, 1)

    def closed(resident_in, project_w, output_w, expand_w, reduce_w, gain_one, gain_two):
        return forward(resident_in, project_w, output_w, expand_w, reduce_w, gain_one, gain_two, clip_lengths)
    output, pullback = jax.vjp(closed, resident, project_weight, output_weight, expand_weight, reduce_weight, gain_first, gain_second)
    grads = pullback(cotangent.astype(jnp.float32).T * row_mask)
    input_grad, project_grad, output_grad, expand_grad, reduce_grad, gain_one_grad, gain_two_grad = grads
    scale = 1.0 / math.sqrt(TOKENS)
    pm, pw, pa = update(project_weight, project_moment, project_average, project_grad, RATE_PROJECT * scale)
    om, ow, oa = update(output_weight, output_moment, output_average, output_grad, RATE_OUTPUT * scale)
    em, ew, ea = update(expand_weight, expand_moment, expand_average, expand_grad, RATE_EXPAND * scale)
    rm, rw, ra = update(reduce_weight, reduce_moment, reduce_average, reduce_grad, RATE_REDUCE * scale)
    fm, fw, fa = update(gain_first, first_moment, first_average, gain_one_grad, RATE_GAIN * scale)
    sm, sw, sa = update(gain_second, second_moment, second_average, gain_two_grad, RATE_GAIN * scale)
    return (output.T.astype(jnp.bfloat16), input_grad.T, project_grad, pm, pw, pa, pw.astype(jnp.bfloat16), output_grad, om, ow, oa, ow.astype(jnp.bfloat16), expand_grad, em, ew, ea, ew.astype(jnp.bfloat16), reduce_grad, rm, rw, ra, rw.astype(jnp.bfloat16), gain_one_grad, fm, fw, fa, gain_two_grad, sm, sw, sa)
```

```python
import functools
import math

import jax
import jax.numpy as jnp
from jax import lax
from jax.experimental import pallas as pl
from jax.experimental.pallas import tpu as pltpu
from jax.sharding import Mesh
from jax.sharding import PartitionSpec as P

HEAD_DIM = 80


EPS = 1e-05
NEG = -1e30
MOMENTUM = 0.9
AVERAGING = 0.6
RATE_PROJECT = 0.07
RATE_OUTPUT = 3.5
RATE_EXPAND = 0.06
RATE_REDUCE = 0.015
RATE_GAIN = 0.2

CLIPS_PER_COLUMN = 4
ROW = ("pair", "core")
COL = ("zhi", "zlo")
COLUMN = ("core", "zhi", "zlo")
TEAM = ("core", "zlo")
EVERY = ("zhi", "zlo", "pair", "core")
SPARE = 16


def exchange(values, axes, step, size):
    return lax.ppermute(values, axes, [(at, at ^ step) for at in range(size)])


def column_pairs(depth, step):
    team = depth // 2
    half = team // 2
    pairs = []
    for core in range(2):
        for place in range(depth):
            chunk = place ^ step
            clip, slot = divmod(chunk, team)
            to_core, low = divmod(slot, half)
            to_place = (2 * core + clip) * (depth // CLIPS_PER_COLUMN) + low
            pairs.append((core * depth + place, to_core * depth + to_place))
    return pairs


def own_chunk(depth):
    team = depth // 2
    place = lax.axis_index(COL)
    per_clip = depth // CLIPS_PER_COLUMN
    clip = (place // per_clip) % 2
    slot = lax.axis_index("core") * (team // 2) + place % per_clip
    return clip * team + slot


def to_tokens(values, depth):
    width, rows = values.shape
    size = rows // depth
    place = lax.axis_index(COL)
    mine = own_chunk(depth)
    pieces = []
    for step in range(depth):
        chunk = lax.dynamic_slice_in_dim(values, (place ^ step) * size, size, 1)
        pieces.append(lax.ppermute(chunk, COLUMN, column_pairs(depth, step)))
    stacked = jnp.stack(pieces)
    order = [lax.dynamic_index_in_dim(stacked, at ^ mine, 0, False) for at in range(depth)]
    return jnp.concatenate(order, axis=0)


def to_features(values, depth):
    width, size = values.shape
    block = width // depth
    place = lax.axis_index(COL)
    mine = own_chunk(depth)
    whole = jnp.zeros((block, size * depth), values.dtype)
    for step in range(depth):
        chunk = lax.dynamic_slice_in_dim(values, (mine ^ step) * block, block, 0)
        back = [(target, source) for source, target in column_pairs(depth, step)]
        piece = lax.ppermute(chunk, COLUMN, back)
        whole = lax.dynamic_update_slice_in_dim(whole, piece, (place ^ step) * size, 1)
    return whole


def attend_kernel(team, valid_ref, *refs):
    query_ref, keys, values = refs[0], refs[1 : 1 + team], refs[1 + team : 1 + 2 * team]
    out_ref, log_ref, wide_keys, wide_values = refs[1 + 2 * team :]
    dim, size = query_ref.shape
    scale = math.log2(math.e) / math.sqrt(HEAD_DIM)
    pad = (SPARE, size)
    row = lax.broadcasted_iota(jnp.int32, pad, 0)
    position = lax.broadcasted_iota(jnp.int32, pad, 1)
    for at in range(team):
        own = keys[at][...]
        bias = jnp.where((row == 0) & (position >= valid_ref[at]), NEG, 0.0).astype(jnp.bfloat16)
        wide = jnp.concatenate([own, own, bias], axis=0)
        wide_keys[pl.ds(at * size, size), :] = wide.T
        ones = jnp.where(row == 0, 1.0, 0.0).astype(jnp.bfloat16)
        wide_values[:, pl.ds(at * size, size)] = jnp.concatenate([values[at][...], ones], axis=0)
    block = 256 if size % 256 == 0 else 128
    for start in range(0, size, block):
        query = query_ref[:, pl.ds(start, block)].astype(jnp.float32) * scale
        high = query.astype(jnp.bfloat16)
        low = (query - high.astype(jnp.float32)).astype(jnp.bfloat16)
        one = jnp.where(
            lax.broadcasted_iota(jnp.int32, (SPARE, block), 0) == 0, 1.0, 0.0
        ).astype(jnp.bfloat16)
        wide_query = jnp.concatenate([high, low, one], axis=0)
        scores = jnp.dot(wide_keys[...], wide_query, preferred_element_type=jnp.float32)
        highest = jnp.max(scores, axis=0, keepdims=True)
        powers = jnp.exp2(scores - highest).astype(jnp.bfloat16)
        mixed = jnp.dot(wide_values[...], powers, preferred_element_type=jnp.float32)
        total = mixed[dim : dim + 1]
        out_ref[:, pl.ds(start, block)] = (mixed[:dim] / total).astype(jnp.bfloat16)
        log_ref[0, :, pl.ds(start, block)] = highest + jnp.log2(total)


def three_parts(values):
    high = values.astype(jnp.bfloat16)
    rest = values - high.astype(jnp.float32)
    middle = rest.astype(jnp.bfloat16)
    low = (rest - middle.astype(jnp.float32)).astype(jnp.bfloat16)
    return high, middle, low


def spare_rows(first, parts, block):
    row = lax.broadcasted_iota(jnp.int32, (SPARE, block), 0)
    rows = jnp.where(row == 0, first, 0.0)
    for at, part in enumerate(parts):
        rows = jnp.where(row == at + 1, -part.astype(jnp.float32), rows)
    return rows.astype(jnp.bfloat16)


def attend_back_kernel(team, valid_ref, *refs):
    query_ref, out_ref, grad_ref, log_ref = refs[:4]
    keys, values = refs[4 : 4 + team], refs[4 + team : 4 + 2 * team]
    query_grad_ref = refs[4 + 2 * team]
    key_grads = refs[5 + 2 * team : 5 + 3 * team]
    value_grads = refs[5 + 3 * team : 5 + 4 * team]
    wide_keys, wide_values, flat_keys, key_total, value_total = refs[5 + 4 * team :]
    dim, size = query_ref.shape
    base = 1.0 / math.sqrt(HEAD_DIM)
    scale = math.log2(math.e) * base
    pad = (SPARE, size)
    row = lax.broadcasted_iota(jnp.int32, pad, 0)
    position = lax.broadcasted_iota(jnp.int32, pad, 1)
    for at in range(team):
        own = keys[at][...]
        outside = position >= valid_ref[at]
        bias = jnp.where(
            row == 0, jnp.where(outside, NEG, 0.0), jnp.where(row < 4, 1.0, 0.0)
        ).astype(jnp.bfloat16)
        wide_keys[pl.ds(at * size, size), :] = jnp.concatenate([own, own, bias], axis=0).T
        flat_keys[:, pl.ds(at * size, size)] = own
        ones = jnp.where((row >= 1) & (row < 4), 1.0, 0.0).astype(jnp.bfloat16)
        wide_values[pl.ds(at * size, size), :] = jnp.concatenate(
            [values[at][...], ones], axis=0
        ).T
    block = 256 if size % 256 == 0 else 128
    for start in range(0, size, block):
        here = pl.ds(start, block)
        raw = query_ref[:, here]
        query = raw.astype(jnp.float32) * scale
        high = query.astype(jnp.bfloat16)
        low = (query - high.astype(jnp.float32)).astype(jnp.bfloat16)
        grad = grad_ref[:, here]
        inner = jnp.sum(
            grad.astype(jnp.float32) * out_ref[:, here].astype(jnp.float32), axis=0, keepdims=True
        )
        wide_query = jnp.concatenate(
            [high, low, spare_rows(1.0, three_parts(log_ref[0, :, here]), block)], axis=0
        )
        wide_grad = jnp.concatenate([grad, spare_rows(0.0, three_parts(inner), block)], axis=0)
        scores = jnp.dot(wide_keys[...], wide_query, preferred_element_type=jnp.float32)
        probs = jnp.exp2(scores)
        prob_grad = jnp.dot(wide_values[...], wide_grad, preferred_element_type=jnp.float32)
        score_grad = (probs * prob_grad).astype(jnp.bfloat16)
        probs = probs.astype(jnp.bfloat16)
        query_grad_ref[:, here] = (
            jnp.dot(flat_keys[...], score_grad, preferred_element_type=jnp.float32) * base
        ).astype(jnp.bfloat16)
        value_part = jnp.dot(probs, grad.T, preferred_element_type=jnp.float32)
        key_part = jnp.dot(score_grad, raw.T, preferred_element_type=jnp.float32)
        if start == 0:
            value_total[...] = value_part
            key_total[...] = key_part
        else:
            value_total[...] += value_part
            key_total[...] += key_part
    for at in range(team):
        part = pl.ds(at * size, size)
        key_grads[at][...] = (key_total[part, :] * base).T.astype(jnp.bfloat16)
        value_grads[at][...] = value_total[part, :].T.astype(jnp.bfloat16)


def head_specs(size, count):
    return [pl.BlockSpec((HEAD_DIM, size), lambda head, *_: (head, 0)) for _ in range(count)]


def attend(query, keys, values, valid):
    width, size = query.shape
    team = len(keys)
    heads = width // HEAD_DIM
    span = team * size
    row_spec = pl.BlockSpec((1, 1, size), lambda head, *_: (head, 0, 0))
    return pl.pallas_call(
        functools.partial(attend_kernel, team),
        out_shape=(
            jax.ShapeDtypeStruct((width, size), jnp.bfloat16),
            jax.ShapeDtypeStruct((heads, 1, size), jnp.float32),
        ),
        grid_spec=pltpu.PrefetchScalarGridSpec(
            num_scalar_prefetch=1,
            grid=(heads,),
            in_specs=head_specs(size, 1 + 2 * team),
            out_specs=(head_specs(size, 1)[0], row_spec),
            scratch_shapes=[
                pltpu.VMEM((span, 2 * HEAD_DIM + SPARE), jnp.bfloat16),
                pltpu.VMEM((HEAD_DIM + SPARE, span), jnp.bfloat16),
            ],
        ),
        cost_estimate=pl.CostEstimate(
            flops=4 * width * size * span,
            bytes_accessed=2 * width * size * (2 + 2 * team),
            transcendentals=heads * size * span,
        ),
        name="attend",
    )(valid, query, *keys, *values)


def attend_back(query, out, grad, logs, keys, values, valid):
    width, size = query.shape
    team = len(keys)
    heads = width // HEAD_DIM
    span = team * size
    row_spec = pl.BlockSpec((1, 1, size), lambda head, *_: (head, 0, 0))
    shape = jax.ShapeDtypeStruct((width, size), jnp.bfloat16)
    results = pl.pallas_call(
        functools.partial(attend_back_kernel, team),
        out_shape=(shape,) * (1 + 2 * team),
        grid_spec=pltpu.PrefetchScalarGridSpec(
            num_scalar_prefetch=1,
            grid=(heads,),
            in_specs=head_specs(size, 3) + [row_spec] + head_specs(size, 2 * team),
            out_specs=head_specs(size, 1 + 2 * team),
            scratch_shapes=[
                pltpu.VMEM((span, 2 * HEAD_DIM + SPARE), jnp.bfloat16),
                pltpu.VMEM((span, HEAD_DIM + SPARE), jnp.bfloat16),
                pltpu.VMEM((HEAD_DIM, span), jnp.bfloat16),
                pltpu.VMEM((span, HEAD_DIM), jnp.float32),
                pltpu.VMEM((span, HEAD_DIM), jnp.float32),
            ],
        ),
        cost_estimate=pl.CostEstimate(
            flops=10 * width * size * span,
            bytes_accessed=2 * width * size * (4 + 4 * team),
            transcendentals=heads * size * span,
        ),
        name="attend_back",
    )(valid, query, out, grad, logs, *keys, *values)
    return results[0], results[1 : 1 + team], results[1 + team :]


def normalize(values):
    average = jnp.mean(values, axis=0, keepdims=True)
    inverse = lax.rsqrt(jnp.mean(values * values, axis=0, keepdims=True) - average * average + EPS)
    return ((values - average) * inverse, inverse)


def normalize_back(incoming, normed, inverse, gain):
    scaled = incoming * gain[:, None]
    total = jnp.mean(scaled, axis=0, keepdims=True)
    crossed = jnp.mean(scaled * normed, axis=0, keepdims=True)
    outgoing = inverse * (scaled - total - normed * crossed)
    return (outgoing, jnp.sum(incoming * normed, axis=1))


def gelu_parts(values):
    inside = 0.5 + 0.5 * lax.erf(values * math.sqrt(0.5))
    density = jnp.exp(-0.5 * values * values) * (1.0 / math.sqrt(2.0 * math.pi))
    return values * inside, inside + values * density


def product(spec, former, latter, kind=jnp.float32):
    return jnp.einsum(spec, former, latter, preferred_element_type=jnp.float32).astype(kind)


def update(weight, moment, average, gradient, rate):
    moment_next = MOMENTUM * moment + gradient
    weight_next = weight - rate * (gradient + MOMENTUM * moment_next)
    average_next = AVERAGING * average + (1.0 - AVERAGING) * weight_next
    return (moment_next, weight_next, average_next)


def gather_weight(shard, depth):
    whole = lax.all_gather(shard, EVERY, axis=0, tiled=True)
    return whole.reshape(depth, whole.shape[0] // depth, shard.shape[1])


def scatter_grad(parts):
    depth, width, columns = parts.shape
    return lax.psum_scatter(
        parts.reshape(depth * width, columns), EVERY, scatter_dimension=0, tiled=True
    ).astype(jnp.float32)


def on_device(
    inputs,
    cotangent,
    clip_lengths,
    project_weight,
    project_moment,
    project_average,
    output_weight,
    output_moment,
    output_average,
    expand_weight,
    expand_moment,
    expand_average,
    reduce_weight,
    reduce_moment,
    reduce_average,
    gain_first,
    first_moment,
    first_average,
    gain_second,
    second_moment,
    second_average,
):
    block_width, rows_local = inputs.shape
    depth = lax.axis_size(COL)
    team = depth // 2
    rows_of_weight = project_weight.shape[1]
    width = block_width * depth
    size = rows_local // depth
    bf16 = jnp.bfloat16

    project_full = gather_weight(
        project_weight.astype(bf16).transpose(1, 0, 2).reshape(rows_of_weight, 3 * block_width),
        depth,
    )
    output_full = gather_weight(output_weight.astype(bf16).T, depth)
    expand_full = gather_weight(expand_weight.astype(bf16), depth)
    reduce_full = gather_weight(reduce_weight.astype(bf16).T, depth)
    gains = lax.all_gather(jnp.stack([gain_first, gain_second]), COL, axis=1, tiled=True)
    lengths = lax.all_gather(clip_lengths, "core", axis=0, tiled=True)

    clip = lax.axis_index("zhi")
    length = lax.dynamic_index_in_dim(lengths, clip, 0, False)
    slot = lax.axis_index(TEAM)
    valid = jnp.clip(
        jnp.stack([length - (slot ^ step) * size for step in range(team)]), 0, size
    ).astype(jnp.int32)
    token_mask = (jnp.arange(size, dtype=jnp.int32) < valid[0]).astype(jnp.float32)[None, :]

    resident = to_tokens(inputs, depth).astype(jnp.float32)
    normed_one, inverse_one = normalize(resident)
    hidden_one = (normed_one * gains[0][:, None]).astype(bf16)
    projected = product(
        "zdke,dt->kzet",
        project_full.reshape(depth, width, 3, block_width),
        hidden_one,
        bf16,
    ).reshape(3, width, size)
    query = projected[0]
    both = projected[1:]
    others = [exchange(both, TEAM, step, team) for step in range(1, team)]
    keys = [both[0]] + [other[0] for other in others]
    values = [both[1]] + [other[1] for other in others]
    attended, logs = attend(query, keys, values, valid)
    middle = resident + product(
        "zde,zet->dt", output_full, attended.reshape(depth, block_width, size)
    )
    normed_two, inverse_two = normalize(middle)
    hidden_two = (normed_two * gains[1][:, None]).astype(bf16)
    pre_act = product("zdu,dt->zut", expand_full, hidden_two)
    activated, slope = gelu_parts(pre_act)
    activated, slope = activated.astype(bf16), slope.astype(bf16)
    block_output = to_features(
        (middle + product("zdu,zut->dt", reduce_full, activated)).astype(bf16), depth
    )

    upstream_low = to_tokens(cotangent, depth) * token_mask.astype(bf16)
    upstream = upstream_low.astype(jnp.float32)
    reduce_grad = scatter_grad(product("dt,zut->zdu", upstream_low, activated, bf16)).T
    pre_grad = (
        product("zdu,dt->zut", reduce_full, upstream_low) * slope.astype(jnp.float32)
    ).astype(bf16)
    expand_grad = scatter_grad(product("dt,zut->zdu", hidden_two, pre_grad, bf16))
    normed_two_grad = product("zdu,zut->dt", expand_full, pre_grad)
    middle_grad, gain_two_part = normalize_back(normed_two_grad, normed_two, inverse_two, gains[1])
    middle_grad = middle_grad + upstream
    middle_grad_low = middle_grad.astype(bf16)
    output_grad = scatter_grad(
        product(
            "dt,zet->zde", middle_grad_low, attended.reshape(depth, block_width, size), bf16
        )
    ).T
    attended_grad = product("zde,dt->zet", output_full, middle_grad_low, bf16).reshape(width, size)
    query_grad, key_grads, value_grads = attend_back(
        query, attended, attended_grad, logs, keys, values, valid
    )
    pair_grad = jnp.stack([key_grads[0], value_grads[0]]).astype(jnp.float32)
    for step in range(1, team):
        pair_grad = pair_grad + exchange(
            jnp.stack([key_grads[step], value_grads[step]]), TEAM, step, team
        ).astype(jnp.float32)
    stacked = jnp.concatenate([query_grad[None], pair_grad.astype(bf16)]).reshape(
        3, depth, block_width, size
    )
    project_grad = scatter_grad(
        product("dt,kzet->zdke", hidden_one, stacked, bf16).reshape(depth, width, 3 * block_width)
    )
    project_grad = project_grad.reshape(rows_of_weight, 3, block_width).transpose(1, 0, 2)
    normed_one_grad = product(
        "zdke,kzet->dt", project_full.reshape(depth, width, 3, block_width), stacked
    )
    input_grad, gain_one_part = normalize_back(normed_one_grad, normed_one, inverse_one, gains[0])
    input_grad = to_features((input_grad + middle_grad).astype(bf16), depth).astype(jnp.float32)
    gain_grads = lax.psum_scatter(
        lax.psum(jnp.stack([gain_one_part, gain_two_part]), ROW), COL, scatter_dimension=1, tiled=True
    )
    gain_one_grad, gain_two_grad = gain_grads[0], gain_grads[1]

    scale = 1.0 / math.sqrt(rows_local * lax.axis_size(ROW))
    pm, pw, pa = update(
        project_weight, project_moment, project_average, project_grad, RATE_PROJECT * scale
    )
    om, ow, oa = update(
        output_weight, output_moment, output_average, output_grad, RATE_OUTPUT * scale
    )
    em, ew, ea = update(
        expand_weight, expand_moment, expand_average, expand_grad, RATE_EXPAND * scale
    )
    rm, rw, ra = update(
        reduce_weight, reduce_moment, reduce_average, reduce_grad, RATE_REDUCE * scale
    )
    fm, fw, fa = update(gain_first, first_moment, first_average, gain_one_grad, RATE_GAIN * scale)
    sm, sw, sa = update(
        gain_second, second_moment, second_average, gain_two_grad, RATE_GAIN * scale
    )
    return (
        block_output,
        input_grad,
        project_grad,
        pm,
        pw,
        pa,
        pw.astype(bf16),
        output_grad,
        om,
        ow,
        oa,
        ow.astype(bf16),
        expand_grad,
        em,
        ew,
        ea,
        ew.astype(bf16),
        reduce_grad,
        rm,
        rw,
        ra,
        rw.astype(bf16),
        gain_one_grad,
        fm,
        fw,
        fa,
        gain_two_grad,
        sm,
        sw,
        sa,
    )


def solution(mesh):
    rows, columns = mesh.shape["row"], mesh.shape["col"]
    finer = Mesh(
        mesh.devices.reshape(rows // 2, 2, CLIPS_PER_COLUMN, columns // CLIPS_PER_COLUMN),
        ("pair", "core", "zhi", "zlo"),
    )
    plane = P(COL, ROW)
    weights = (P(None, ROW, COL), plane, P(ROW, COL), plane)
    placed = (plane, plane, P(ROW))
    for spec in weights:
        placed += (spec,) * 3
    placed += (P(COL),) * 6
    results = (plane, plane)
    for spec in weights:
        results += (spec,) * 5
    results += (P(COL),) * 8
    return jax.shard_map(
        on_device, mesh=finer, in_specs=placed, out_specs=results, check_vma=False
    )
```

```python
import functools
import math

import jax
import jax.numpy as jnp
from jax import lax
from jax.experimental import pallas as pl
from jax.experimental.pallas import tpu as pltpu
from jax.sharding import Mesh
from jax.sharding import PartitionSpec as P

HEAD_DIM = 80


EPS = 1e-05
NEG = -1e30
MOMENTUM = 0.9
AVERAGING = 0.6
RATE_PROJECT = 0.07
RATE_OUTPUT = 3.5
RATE_EXPAND = 0.06
RATE_REDUCE = 0.015
RATE_GAIN = 0.2

CLIPS_PER_COLUMN = 4
ROW = ("pair", "core")
COL = ("zhi", "zlo")
COLUMN = ("core", "zhi", "zlo")
TEAM = ("core", "zlo")
EVERY = ("zhi", "zlo", "pair", "core")
SPARE = 16


def exchange(values, axes, step, size):
    return lax.ppermute(values, axes, [(at, at ^ step) for at in range(size)])


def column_pairs(depth, step):
    team = depth // 2
    half = team // 2
    pairs = []
    for core in range(2):
        for place in range(depth):
            chunk = place ^ step
            clip, slot = divmod(chunk, team)
            to_core, low = divmod(slot, half)
            to_place = (2 * core + clip) * (depth // CLIPS_PER_COLUMN) + low
            pairs.append((core * depth + place, to_core * depth + to_place))
    return pairs


def own_chunk(depth):
    team = depth // 2
    place = lax.axis_index(COL)
    per_clip = depth // CLIPS_PER_COLUMN
    clip = (place // per_clip) % 2
    slot = lax.axis_index("core") * (team // 2) + place % per_clip
    return clip * team + slot


def to_tokens(values, depth):
    width, rows = values.shape
    size = rows // depth
    place = lax.axis_index(COL)
    mine = own_chunk(depth)
    pieces = []
    for step in range(depth):
        chunk = lax.dynamic_slice_in_dim(values, (place ^ step) * size, size, 1)
        pieces.append(lax.ppermute(chunk, COLUMN, column_pairs(depth, step)))
    stacked = jnp.stack(pieces)
    order = [lax.dynamic_index_in_dim(stacked, at ^ mine, 0, False) for at in range(depth)]
    return jnp.concatenate(order, axis=0)


def to_features(values, depth):
    width, size = values.shape
    block = width // depth
    place = lax.axis_index(COL)
    mine = own_chunk(depth)
    whole = jnp.zeros((block, size * depth), values.dtype)
    for step in range(depth):
        chunk = lax.dynamic_slice_in_dim(values, (mine ^ step) * block, block, 0)
        back = [(target, source) for source, target in column_pairs(depth, step)]
        piece = lax.ppermute(chunk, COLUMN, back)
        whole = lax.dynamic_update_slice_in_dim(whole, piece, (place ^ step) * size, 1)
    return whole


MESH_ID = pl.DeviceIdType.MESH


def places():
    return (
        lax.axis_index("pair"),
        lax.axis_index("core"),
        lax.axis_index("zhi"),
    )


def device(pair, core, place):
    return (pair, core, place, 0)


def greet(pair, core, place):
    barrier = pltpu.get_barrier_semaphore()
    others = [device(pair ^ 1, core, place), device(pair ^ 2, core, place)]
    for flip in range(2):
        for step in range(CLIPS_PER_COLUMN):
            if flip or step:
                others.append(device(pair, core ^ flip, place ^ step))
    for other in others:
        pl.semaphore_signal(barrier, inc=1, device_id=other, device_id_type=MESH_ID)
    pl.semaphore_wait(barrier, len(others))


def gather_kernel(groups, values_ref, gain_ref, *refs):
    shards, wholes = refs[:groups], refs[groups + 2 : 2 * groups + 2]
    tokens_ref, gains_ref = refs[groups : groups + 2]
    (x_send, x_recv, g_send, g_recv, own_sem, z_send, z_recv, p_send, p_recv, c_send, c_recv) = (
        refs[2 * groups + 2 :]
    )
    pair, core, place = places()
    row = 2 * pair + core
    depth = CLIPS_PER_COLUMN
    block, rows = values_ref.shape
    size = rows // depth
    greet(pair, core, place)

    def remote(source, target, send, recv, where):
        return pltpu.make_async_remote_copy(
            src_ref=source,
            dst_ref=target,
            send_sem=send,
            recv_sem=recv,
            device_id=where,
            device_id_type=MESH_ID,
        )

    mine = (place % 2) * 2 + core
    targets = []
    for step in range(depth):
        chunk = place ^ step
        to_core, to_place = chunk % 2, 2 * core + chunk // 2
        source = values_ref.at[:, pl.ds(pl.multiple_of(chunk * size, size), size)]
        home = tokens_ref.at[place]
        away = (to_core != core) | (to_place != place)
        copy = remote(
            source, home, x_send.at[step], x_recv.at[step], device(pair, to_core, to_place)
        )
        local = pltpu.make_async_copy(source, home, x_recv.at[step])
        targets.append((away, copy, local))

        @pl.when(away)
        def _():
            copy.start()

        @pl.when(jnp.logical_not(away))
        def _():
            local.start()

    def piece(group, step, other, flip):
        return wholes[group].at[place ^ step, 2 * (pair ^ other) + (core ^ flip)]

    own = [
        pltpu.make_async_copy(shards[group], piece(group, 0, 0, 0), own_sem.at[group])
        for group in range(groups)
    ]
    sends = []
    own.append(pltpu.make_async_copy(gain_ref, gains_ref.at[place], g_recv.at[0]))
    for step in range(1, depth):
        copy = remote(
            gain_ref,
            gains_ref.at[place],
            g_send.at[step],
            g_recv.at[step],
            device(pair, core, place ^ step),
        )
        copy.start()
        sends.append(copy)
    for group in range(groups):
        for step in range(1, depth):
            copy = remote(
                shards[group],
                wholes[group].at[place, row],
                z_send.at[group, step],
                z_recv.at[group, step],
                device(pair, core, place ^ step),
            )
            copy.start()
            sends.append(copy)
    for copy in own:
        copy.start()

    def to_pair(group, step, other, hop, slot):
        source = (
            shards[group] if step == 0 and other == 0 else piece(group, step, other, 0)
        )
        copy = remote(
            source,
            piece(group, step, other, 0),
            p_send.at[group, step, slot],
            p_recv.at[group, step, other ^ hop],
            device(pair ^ hop, core, place),
        )
        copy.start()
        sends.append(copy)

    def to_core(group, step, other):
        source = (
            shards[group] if step == 0 and other == 0 else piece(group, step, other, 0)
        )
        copy = remote(
            source,
            piece(group, step, other, 0),
            c_send.at[group, step, other],
            c_recv.at[group, step, other],
            device(pair, core ^ 1, place),
        )
        copy.start()
        sends.append(copy)

    def await_piece(group, step, other, flip, sem):
        here = piece(group, step, other, flip)
        remote(here, here, sem, sem, device(pair ^ 1, core, place)).wait_recv()

    order = [(group, step) for step in range(depth) for group in range(groups)]

    def first_hop(group, step):
        if step:
            await_piece(group, step, 0, 0, z_recv.at[group, step])
        near, far = (1, 2) if (group + step) % 2 == 0 else (2, 1)
        to_pair(group, step, 0, near, 0)
        to_pair(group, step, 0, far, 1)
        to_core(group, step, 0)

    def second_hop(group, step):
        near, far = (1, 2) if (group + step) % 2 == 0 else (2, 1)
        await_piece(group, step, near, 0, p_recv.at[group, step, near])
        to_pair(group, step, near, far, 2)
        to_core(group, step, near)

    def last_hop(group, step):
        near, far = (1, 2) if (group + step) % 2 == 0 else (2, 1)
        for other in (far, 3):
            await_piece(group, step, other, 0, p_recv.at[group, step, other])
            to_core(group, step, other)

    for at in range(len(order) + 4):
        if at < len(order):
            first_hop(*order[at])
        if 0 <= at - 2 < len(order):
            second_hop(*order[at - 2])
        if 0 <= at - 4:
            last_hop(*order[at - 4])
    for group, step in order:
        for other in range(4):
            await_piece(group, step, other, 1, c_recv.at[group, step, other])
    for step in range(1, depth):
        here = gains_ref.at[place ^ step]
        remote(
            here, here, g_recv.at[step], g_recv.at[step], device(pair, core ^ 1, place)
        ).wait_recv()
    for copy in own:
        copy.wait()
    for copy in sends:
        copy.wait_send()
    for step in range(depth):
        away, copy, local = targets[step]
        home = tokens_ref.at[place]
        from_core, from_place = place // 2, mine ^ step
        foreign = (from_core != core) | (from_place != place)

        @pl.when(foreign)
        def _():
            remote(
                home, home, x_recv.at[step], x_recv.at[step], device(pair, core ^ 1, place)
            ).wait_recv()

        @pl.when(jnp.logical_not(foreign))
        def _():
            pltpu.make_async_copy(home, home, x_recv.at[step]).wait()

        @pl.when(away)
        def _():
            copy.wait_send()


def gather_all(values, gain, shards):
    groups = len(shards)
    depth = CLIPS_PER_COLUMN
    block, rows = values.shape
    size = rows // depth
    dma = pltpu.SemaphoreType.DMA
    anywhere = pl.BlockSpec(memory_space=pl.ANY)
    results = pl.pallas_call(
        functools.partial(gather_kernel, groups),
        out_shape=[
            jax.ShapeDtypeStruct((depth, block, size), values.dtype),
            jax.ShapeDtypeStruct((depth, *gain.shape), gain.dtype),
        ]
        + [
            jax.ShapeDtypeStruct((depth, 2 * 4, *shard.shape), shard.dtype) for shard in shards
        ],
        in_specs=[anywhere] * (2 + groups),
        out_specs=[anywhere] * (2 + groups),
        scratch_shapes=[
            dma((depth,)),
            dma((depth,)),
            dma((depth,)),
            dma((depth,)),
            dma((groups,)),
            dma((groups, depth)),
            dma((groups, depth)),
            dma((groups, depth, 3)),
            dma((groups, depth, 4)),
            dma((groups, depth, 4)),
            dma((groups, depth, 4)),
        ],
        compiler_params=pltpu.CompilerParams(collective_id=1, has_side_effects=True),
        name="gather_all",
    )(values, gain, *shards)
    return results[0], results[1], results[2:]


def add_into(total, part):
    rows = total.shape[0]
    step = 32 if rows % 32 == 0 else 16

    @pl.loop(0, rows // step)
    def _(at):
        here = pl.ds(pl.multiple_of(at * step, step), step)
        total[here, :] = (
            total[here, :].astype(jnp.float32) + part[here, :].astype(jnp.float32)
        ).astype(total.dtype)


def scatter_kernel(groups, values_ref, gain_ref, *refs):
    parts, refs = refs[:groups], refs[groups:]
    rows_ref, gain_out = refs[:2]
    outs, refs = refs[2 : 2 + groups], refs[2 + groups :]
    halves = refs[:groups]
    passed = refs[groups : 2 * groups]
    landed = refs[2 * groups : 3 * groups]
    staged = refs[3 * groups : 4 * groups]
    gain_sum, gain_in = refs[4 * groups : 4 * groups + 2]
    (x_send, x_recv, g_send, g_recv, l_sem, c_send, c_recv, p_send, p_recv, z_send, z_recv) = refs[
        4 * groups + 2 :
    ]
    pair, core, place = places()
    depth = CLIPS_PER_COLUMN
    greet(pair, core, place)

    def remote(source, target, send, recv, where):
        return pltpu.make_async_remote_copy(
            src_ref=source,
            dst_ref=target,
            send_sem=send,
            recv_sem=recv,
            device_id=where,
            device_id_type=MESH_ID,
        )

    sends = []

    def send(source, target, send_sem, recv_sem, where):
        copy = remote(source, target, send_sem, recv_sem, where)
        copy.start()
        sends.append(copy)

    def arrived(target, sem):
        remote(target, target, sem, sem, device(pair ^ 1, core, place)).wait_recv()

    def block(group, step, other, flip):
        return parts[group].at[place ^ step, 2 * (pair ^ other) + (core ^ flip)]

    mine = (place % 2) * 2 + core
    block_width = rows_ref.shape[0]
    size = values_ref.shape[1]
    moves = []
    for step in range(depth):
        to_core, to_place = place // 2, mine ^ step
        source = values_ref.at[
            pl.ds(pl.multiple_of(to_place * block_width, block_width), block_width), :
        ]
        target = rows_ref.at[:, pl.ds(pl.multiple_of(mine * size, size), size)]
        copy = remote(
            source, target, x_send.at[step], x_recv.at[step], device(pair, to_core, to_place)
        )
        local = pltpu.make_async_copy(source, target, x_recv.at[step])
        away = (to_core != core) | (to_place != place)
        moves.append((away, copy))

        @pl.when(away)
        def _():
            copy.start()

        @pl.when(jnp.logical_not(away))
        def _():
            local.start()

    for step in range(1, depth):
        send(
            gain_ref.at[place ^ step],
            gain_in.at[step],
            g_send.at[step],
            g_recv.at[step],
            device(pair, core, place ^ step),
        )

    def gain_column():
        total = gain_ref[place]
        for step in range(1, depth):
            arrived(gain_in.at[step], g_recv.at[step])
            total += gain_in[step]
        gain_sum[0] = total
        gain_hop(0)

    def gain_hop(at):
        send(
            gain_sum.at[at],
            gain_in.at[depth + at],
            g_send.at[depth + at],
            g_recv.at[depth + at],
            [
                device(pair, core ^ 1, place),
                device(pair ^ 1, core, place),
                device(pair ^ 2, core, place),
            ][at],
        )

    def gain_land(at):
        arrived(gain_in.at[depth + at], g_recv.at[depth + at])
        total = gain_sum[at] + gain_in[depth + at]
        if at < 2:
            gain_sum[at + 1] = total
            gain_hop(at + 1)
        else:
            gain_out[...] = total

    order = [(group, step) for step in (1, 2, 3, 0) for group in range(groups)]
    for group, step in order:
        for other in range(4):
            send(
                block(group, step, other, 1),
                halves[group].at[step, other],
                c_send.at[group, step, other],
                c_recv.at[group, step, other],
                device(pair, core ^ 1, place),
            )

    def load(at):
        group, step = order[at]
        copies = []
        for other in range(4):
            copy = pltpu.make_async_copy(
                block(group, step, other, 0),
                staged[group].at[step % 2, other],
                l_sem.at[group, step % 2, other],
            )
            copy.start()
            copies.append(copy)
        return copies

    def ways(group, step):
        return (1, 2) if (group + step) % 2 == 0 else (2, 1)

    def first_hop(group, step, loads):
        near, far = ways(group, step)
        for other in (near, 3, far, 0):
            half = halves[group].at[step, other]
            arrived(half, c_recv.at[group, step, other])
            loads[other].wait()
            add_into(half, staged[group].at[step % 2, other])
            if other == near or other == 3:
                slot = 0 if other == near else 1
                send(
                    half,
                    passed[group].at[step, slot],
                    p_send.at[group, step, slot],
                    p_recv.at[group, step, slot],
                    device(pair ^ near, core, place),
                )

    def second_hop(group, step):
        near, far = ways(group, step)
        arrived(passed[group].at[step, 1], p_recv.at[group, step, 1])
        add_into(halves[group].at[step, far], passed[group].at[step, 1])
        send(
            halves[group].at[step, far],
            passed[group].at[step, 2],
            p_send.at[group, step, 2],
            p_recv.at[group, step, 2],
            device(pair ^ far, core, place),
        )
        arrived(passed[group].at[step, 0], p_recv.at[group, step, 0])
        add_into(halves[group].at[step, 0], passed[group].at[step, 0])

    def last_hop(group, step):
        arrived(passed[group].at[step, 2], p_recv.at[group, step, 2])
        add_into(halves[group].at[step, 0], passed[group].at[step, 2])
        if step:
            send(
                halves[group].at[step, 0],
                landed[group].at[step - 1],
                z_send.at[group, step],
                z_recv.at[group, step],
                device(pair, core, place ^ step),
            )

    loads = {0: load(0)}
    for at in range(len(order) + 4):
        if at + 1 < len(order):
            loads[at + 1] = load(at + 1)
        if at < len(order):
            first_hop(*order[at], loads[at])
        if 0 <= at - 2 < len(order):
            second_hop(*order[at - 2])
        if 0 <= at - 4:
            last_hop(*order[at - 4])
        if at == 2:
            gain_column()
        if at in (4, 6, 8):
            gain_land((at - 4) // 2)
    for group in range(groups):
        for step in range(1, depth):
            arrived(landed[group].at[step - 1], z_recv.at[group, step])
        rows = outs[group].shape[0]
        unit = 32 if rows % 32 == 0 else 16

        @pl.loop(0, rows // unit)
        def _(at):
            here = pl.ds(pl.multiple_of(at * unit, unit), unit)
            total = halves[group][0, 0, here, :].astype(jnp.float32)
            for step in range(1, depth):
                total += landed[group][step - 1, here, :].astype(jnp.float32)
            outs[group][here, :] = total

    for copy in sends:
        copy.wait_send()
    for step in range(depth):
        chunk = place ^ step
        from_core, from_place = chunk % 2, 2 * core + chunk // 2
        target = rows_ref.at[:, pl.ds(pl.multiple_of(chunk * size, size), size)]
        foreign = (from_core != core) | (from_place != place)
        away, copy = moves[step]

        @pl.when(foreign)
        def _():
            arrived(target, x_recv.at[step])

        @pl.when(jnp.logical_not(foreign))
        def _():
            pltpu.make_async_copy(target, target, x_recv.at[step]).wait()

        @pl.when(away)
        def _():
            copy.wait_send()


def scatter_all(values, gain, parts):
    groups = len(parts)
    depth = CLIPS_PER_COLUMN
    width, size = values.shape
    dma = pltpu.SemaphoreType.DMA
    anywhere = pl.BlockSpec(memory_space=pl.ANY)
    inside = pl.BlockSpec(memory_space=pltpu.VMEM)
    shapes = [part.shape[2:] for part in parts]
    low = jnp.bfloat16
    results = pl.pallas_call(
        functools.partial(scatter_kernel, groups),
        out_shape=[
            jax.ShapeDtypeStruct((width // depth, size * depth), values.dtype),
            jax.ShapeDtypeStruct(gain.shape[1:], gain.dtype),
        ]
        + [jax.ShapeDtypeStruct(shape, jnp.float32) for shape in shapes],
        in_specs=[anywhere, inside] + [anywhere] * groups,
        out_specs=[anywhere, inside] + [inside] * groups,
        scratch_shapes=[pltpu.VMEM((depth, 4, *shape), low) for shape in shapes]
        + [pltpu.VMEM((depth, 3, *shape), low) for shape in shapes]
        + [pltpu.VMEM((depth - 1, *shape), low) for shape in shapes]
        + [pltpu.VMEM((2, 4, *shape), low) for shape in shapes]
        + [
            pltpu.VMEM((3, *gain.shape[1:]), gain.dtype),
            pltpu.VMEM((depth + 3, *gain.shape[1:]), gain.dtype),
            dma((depth,)),
            dma((depth,)),
            dma((depth + 3,)),
            dma((depth + 3,)),
            dma((groups, 2, 4)),
            dma((groups, depth, 4)),
            dma((groups, depth, 4)),
            dma((groups, depth, 3)),
            dma((groups, depth, 3)),
            dma((groups, depth)),
            dma((groups, depth)),
        ],
        cost_estimate=pl.CostEstimate(
            flops=200_000_000_000, bytes_accessed=500_000_000, transcendentals=0
        ),
        compiler_params=pltpu.CompilerParams(
            collective_id=2, has_side_effects=True, vmem_limit_bytes=60 << 20
        ),
        name="scatter_all",
    )(values, gain, *parts)
    return results[0], results[1], results[2:]


def outer_kernel(former_ref, latter_ref, out_ref):
    out_ref[0] = lax.dot_general(
        former_ref[...],
        latter_ref[0],
        (((1,), (1,)), ((), ())),
        preferred_element_type=jnp.float32,
    ).astype(out_ref.dtype)


def outer(former, latter):
    width, size = former.shape
    depth, columns, _ = latter.shape
    tile = width // 2
    return pl.pallas_call(
        outer_kernel,
        out_shape=jax.ShapeDtypeStruct((depth, width, columns), jnp.bfloat16),
        grid=(depth, width // tile),
        in_specs=[
            pl.BlockSpec((tile, size), lambda at, row: (row, 0)),
            pl.BlockSpec((1, columns, size), lambda at, row: (at, 0, 0)),
        ],
        out_specs=pl.BlockSpec((1, tile, columns), lambda at, row: (at, row, 0)),
        cost_estimate=pl.CostEstimate(
            flops=2 * depth * width * columns * size,
            bytes_accessed=2 * depth * width * columns,
            transcendentals=0,
        ),
        name="outer",
    )(former, latter)


def gather_every(values, gains, shards, depth):
    count, block = gains.shape
    if paved():
        padded = jnp.pad(gains, ((0, 8 - count), (0, 0)))
        tokens, gains, wholes = gather_all(values, padded, shards)
        tokens = tokens.reshape(-1, tokens.shape[2])
    else:
        tokens = to_tokens(values, depth)
        gains = lax.all_gather(gains, COL, axis=0)
        wholes = [lax.all_gather(shard, EVERY, axis=0, tiled=True) for shard in shards]
    gains = gains[:, :count].transpose(1, 0, 2).reshape(count, depth * block)
    return (
        tokens,
        gains,
        [whole.reshape(depth, -1, shard.shape[1]) for whole, shard in zip(wholes, shards)],
    )


def scatter_every(values, gains, parts, rows, depth):
    count, width = gains.shape
    if paved():
        blocks = gains.reshape(count, depth, width // depth).transpose(1, 0, 2)
        values, gains, sums = scatter_all(
            values,
            jnp.pad(blocks, ((0, 0), (0, 8 - count), (0, 0))),
            [part.reshape(part.shape[0], -1, rows, part.shape[2]) for part in parts],
        )
        return values, gains[:count], sums
    gains = lax.dynamic_slice_in_dim(
        lax.psum(gains, EVERY), lax.axis_index(COL) * (width // depth), width // depth, 1
    )
    return (
        to_features(values, depth),
        gains,
        [
            lax.psum_scatter(
                part.reshape(-1, part.shape[2]), EVERY, scatter_dimension=0, tiled=True
            ).astype(jnp.float32)
            for part in parts
        ],
    )


def paved():
    return lax.axis_size("pair") == 4 and lax.axis_size(COL) == CLIPS_PER_COLUMN


def attend_kernel(team, valid_ref, *refs):
    own_ref, others = refs[0], refs[1:team]
    query_ref = own_ref.at[0, 2, 0]
    keys = [ref.at[0, 0, 0] for ref in (own_ref, *others)]
    values = [ref.at[0, 1, 0] for ref in (own_ref, *others)]
    out_ref, log_ref, wide_keys, wide_values = refs[team:]
    dim, size = query_ref.shape
    scale = math.log2(math.e) / math.sqrt(HEAD_DIM)
    pad = (SPARE, size)
    row = lax.broadcasted_iota(jnp.int32, pad, 0)
    position = lax.broadcasted_iota(jnp.int32, pad, 1)
    for at in range(team):
        own = keys[at][...]
        bias = jnp.where((row == 0) & (position >= valid_ref[at]), NEG, 0.0).astype(jnp.bfloat16)
        wide = jnp.concatenate([own, own, bias], axis=0)
        wide_keys[pl.ds(at * size, size), :] = wide.T
        ones = jnp.where(row == 0, 1.0, 0.0).astype(jnp.bfloat16)
        wide_values[:, pl.ds(at * size, size)] = jnp.concatenate([values[at][...], ones], axis=0)
    block = 256 if size % 256 == 0 else 128
    for start in range(0, size, block):
        query = query_ref[:, pl.ds(start, block)].astype(jnp.float32) * scale
        high = query.astype(jnp.bfloat16)
        low = (query - high.astype(jnp.float32)).astype(jnp.bfloat16)
        one = jnp.where(
            lax.broadcasted_iota(jnp.int32, (SPARE, block), 0) == 0, 1.0, 0.0
        ).astype(jnp.bfloat16)
        wide_query = jnp.concatenate([high, low, one], axis=0)
        scores = jnp.dot(wide_keys[...], wide_query, preferred_element_type=jnp.float32)
        highest = jnp.max(scores, axis=0, keepdims=True)
        powers = jnp.exp2(scores - highest).astype(jnp.bfloat16)
        mixed = jnp.dot(wide_values[...], powers, preferred_element_type=jnp.float32)
        total = mixed[dim : dim + 1]
        out_ref[:, pl.ds(start, block)] = (mixed[:dim] / total).astype(jnp.bfloat16)
        log_ref[0, :, pl.ds(start, block)] = highest + jnp.log2(total)


def three_parts(values):
    high = values.astype(jnp.bfloat16)
    rest = values - high.astype(jnp.float32)
    middle = rest.astype(jnp.bfloat16)
    low = (rest - middle.astype(jnp.float32)).astype(jnp.bfloat16)
    return high, middle, low


def spare_rows(first, parts, block):
    row = lax.broadcasted_iota(jnp.int32, (SPARE, block), 0)
    rows = jnp.where(row == 0, first, 0.0)
    for at, part in enumerate(parts):
        rows = jnp.where(row == at + 1, -part.astype(jnp.float32), rows)
    return rows.astype(jnp.bfloat16)


def attend_back_kernel(team, valid_ref, *refs):
    out_ref, grad_ref, log_ref, own_ref = refs[:4]
    others = refs[4 : 3 + team]
    query_ref = own_ref.at[0, 2, 0]
    keys = [ref.at[0, 0, 0] for ref in (own_ref, *others)]
    values = [ref.at[0, 1, 0] for ref in (own_ref, *others)]
    grads = refs[3 + team : 3 + 2 * team]
    query_grad_ref = grads[0].at[0, 2, 0]
    key_grads = [ref.at[0, 0, 0] for ref in grads]
    value_grads = [ref.at[0, 1, 0] for ref in grads]
    wide_keys, wide_values, flat_keys, key_total, value_total = refs[3 + 2 * team :]
    dim, size = query_ref.shape
    base = 1.0 / math.sqrt(HEAD_DIM)
    scale = math.log2(math.e) * base
    pad = (SPARE, size)
    row = lax.broadcasted_iota(jnp.int32, pad, 0)
    position = lax.broadcasted_iota(jnp.int32, pad, 1)
    for at in range(team):
        own = keys[at][...]
        outside = position >= valid_ref[at]
        bias = jnp.where(
            row == 0, jnp.where(outside, NEG, 0.0), jnp.where(row < 4, 1.0, 0.0)
        ).astype(jnp.bfloat16)
        wide_keys[pl.ds(at * size, size), :] = jnp.concatenate([own, own, bias], axis=0).T
        flat_keys[:, pl.ds(at * size, size)] = own
        ones = jnp.where((row >= 1) & (row < 4), 1.0, 0.0).astype(jnp.bfloat16)
        wide_values[pl.ds(at * size, size), :] = jnp.concatenate(
            [values[at][...], ones], axis=0
        ).T
    block = 256 if size % 256 == 0 else 128
    for start in range(0, size, block):
        here = pl.ds(start, block)
        raw = query_ref[:, here]
        query = raw.astype(jnp.float32) * scale
        high = query.astype(jnp.bfloat16)
        low = (query - high.astype(jnp.float32)).astype(jnp.bfloat16)
        grad = grad_ref[:, here]
        inner = jnp.sum(
            grad.astype(jnp.float32) * out_ref[:, here].astype(jnp.float32), axis=0, keepdims=True
        )
        wide_query = jnp.concatenate(
            [high, low, spare_rows(1.0, three_parts(log_ref[0, :, here]), block)], axis=0
        )
        wide_grad = jnp.concatenate([grad, spare_rows(0.0, three_parts(inner), block)], axis=0)
        scores = jnp.dot(wide_keys[...], wide_query, preferred_element_type=jnp.float32)
        probs = jnp.exp2(scores)
        prob_grad = jnp.dot(wide_values[...], wide_grad, preferred_element_type=jnp.float32)
        score_grad = (probs * prob_grad).astype(jnp.bfloat16)
        probs = probs.astype(jnp.bfloat16)
        query_grad_ref[:, here] = (
            jnp.dot(flat_keys[...], score_grad, preferred_element_type=jnp.float32) * base
        ).astype(jnp.bfloat16)
        value_part = jnp.dot(probs, grad.T, preferred_element_type=jnp.float32)
        key_part = jnp.dot(score_grad, raw.T, preferred_element_type=jnp.float32)
        if start == 0:
            value_total[...] = value_part
            key_total[...] = key_part
        else:
            value_total[...] += value_part
            key_total[...] += key_part
    for at in range(team):
        part = pl.ds(at * size, size)
        key_grads[at][...] = (key_total[part, :] * base).T.astype(jnp.bfloat16)
        value_grads[at][...] = value_total[part, :].T.astype(jnp.bfloat16)


def part_spec(parts, per_block, size):
    return pl.BlockSpec(
        (1, parts, 1, HEAD_DIM, size),
        lambda head, *_: (head // per_block, 0, head % per_block, 0, 0),
    )


def attend(own, others, valid):
    depth, _, per_block, _, size = own.shape
    heads = depth * per_block
    width = heads * HEAD_DIM
    team = 1 + len(others)
    span = team * size
    row_spec = pl.BlockSpec((1, 1, size), lambda head, *_: (head, 0, 0))
    return pl.pallas_call(
        functools.partial(attend_kernel, team),
        out_shape=(
            jax.ShapeDtypeStruct((width, size), jnp.bfloat16),
            jax.ShapeDtypeStruct((heads, 1, size), jnp.float32),
        ),
        grid_spec=pltpu.PrefetchScalarGridSpec(
            num_scalar_prefetch=1,
            grid=(heads,),
            in_specs=[part_spec(3, per_block, size)]
            + [part_spec(2, per_block, size) for _ in others],
            out_specs=(pl.BlockSpec((HEAD_DIM, size), lambda head, *_: (head, 0)), row_spec),
            scratch_shapes=[
                pltpu.VMEM((span, 2 * HEAD_DIM + SPARE), jnp.bfloat16),
                pltpu.VMEM((HEAD_DIM + SPARE, span), jnp.bfloat16),
            ],
        ),
        cost_estimate=pl.CostEstimate(
            flops=12 * width * size * span,
            bytes_accessed=2 * width * size * (2 + 2 * team),
            transcendentals=heads * size * span,
        ),
        name="attend",
    )(valid, own, *others)


def attend_back(own, others, out, grad, logs, valid):
    depth, _, per_block, _, size = own.shape
    heads = depth * per_block
    width = heads * HEAD_DIM
    team = 1 + len(others)
    span = team * size
    row_spec = pl.BlockSpec((1, 1, size), lambda head, *_: (head, 0, 0))
    head_spec = pl.BlockSpec((HEAD_DIM, size), lambda head, *_: (head, 0))
    part_specs = [part_spec(3, per_block, size)] + [part_spec(2, per_block, size) for _ in others]
    results = pl.pallas_call(
        functools.partial(attend_back_kernel, team),
        out_shape=[jax.ShapeDtypeStruct(array.shape, jnp.bfloat16) for array in (own, *others)],
        grid_spec=pltpu.PrefetchScalarGridSpec(
            num_scalar_prefetch=1,
            grid=(heads,),
            in_specs=[head_spec, head_spec, row_spec] + part_specs,
            out_specs=part_specs,
            scratch_shapes=[
                pltpu.VMEM((span, 2 * HEAD_DIM + SPARE), jnp.bfloat16),
                pltpu.VMEM((span, HEAD_DIM + SPARE), jnp.bfloat16),
                pltpu.VMEM((HEAD_DIM, span), jnp.bfloat16),
                pltpu.VMEM((span, HEAD_DIM), jnp.float32),
                pltpu.VMEM((span, HEAD_DIM), jnp.float32),
            ],
        ),
        cost_estimate=pl.CostEstimate(
            flops=30 * width * size * span,
            bytes_accessed=2 * width * size * (4 + 4 * team),
            transcendentals=heads * size * span,
        ),
        name="attend_back",
    )(valid, out, grad, logs, own, *others)
    return results[0], results[1:]


def normalize(values):
    average = jnp.mean(values, axis=0, keepdims=True)
    inverse = lax.rsqrt(jnp.mean(values * values, axis=0, keepdims=True) - average * average + EPS)
    return ((values - average) * inverse, inverse)


def normalize_back(incoming, normed, inverse, gain):
    scaled = incoming * gain[:, None]
    total = jnp.mean(scaled, axis=0, keepdims=True)
    crossed = jnp.mean(scaled * normed, axis=0, keepdims=True)
    outgoing = inverse * (scaled - total - normed * crossed)
    return (outgoing, jnp.sum(incoming * normed, axis=1))


def gelu_parts(values):
    inside = 0.5 + 0.5 * lax.erf(values * math.sqrt(0.5))
    density = jnp.exp(-0.5 * values * values) * (1.0 / math.sqrt(2.0 * math.pi))
    return values * inside, inside + values * density


def product(spec, former, latter, kind=jnp.float32):
    return jnp.einsum(spec, former, latter, preferred_element_type=jnp.float32).astype(kind)


def update(weight, moment, average, gradient, rate):
    moment_next = MOMENTUM * moment + gradient
    weight_next = weight - rate * (gradient + MOMENTUM * moment_next)
    average_next = AVERAGING * average + (1.0 - AVERAGING) * weight_next
    return (moment_next, weight_next, average_next)


def on_device(
    inputs,
    cotangent,
    clip_lengths,
    project_weight,
    project_moment,
    project_average,
    output_weight,
    output_moment,
    output_average,
    expand_weight,
    expand_moment,
    expand_average,
    reduce_weight,
    reduce_moment,
    reduce_average,
    gain_first,
    first_moment,
    first_average,
    gain_second,
    second_moment,
    second_average,
):
    block_width, rows_local = inputs.shape
    depth = lax.axis_size(COL)
    team = depth // 2
    rows_of_weight = project_weight.shape[1]
    width = block_width * depth
    size = rows_local // depth
    per_block = block_width // HEAD_DIM
    bf16 = jnp.bfloat16
    core = lax.axis_index("core")

    shard = project_weight.astype(bf16)
    resident, gains, (project_full, output_full, expand_full, reduce_full) = gather_every(
        inputs,
        jnp.stack([gain_first, gain_second]),
        [
            jnp.concatenate([shard[1], shard[2], shard[0]], axis=1),
            output_weight.astype(bf16).T,
            expand_weight.astype(bf16),
            reduce_weight.astype(bf16).T,
        ],
        depth,
    )
    resident = resident.astype(jnp.float32)

    other_lengths = exchange(clip_lengths, "core", 1, 2)
    lengths = jnp.where(
        core == 0,
        jnp.concatenate([clip_lengths, other_lengths]),
        jnp.concatenate([other_lengths, clip_lengths]),
    )
    length = lax.dynamic_index_in_dim(lengths, lax.axis_index("zhi"), 0, False)
    slot = lax.axis_index(TEAM)
    valid = jnp.clip(
        jnp.stack([length - (slot ^ step) * size for step in range(team)]), 0, size
    ).astype(jnp.int32)
    token_mask = (jnp.arange(size, dtype=jnp.int32) < valid[0]).astype(jnp.float32)[None, :]

    normed_one, inverse_one = normalize(resident)
    hidden_one = (normed_one * gains[0][:, None]).astype(bf16)
    own = product("zdu,dt->zut", project_full, hidden_one, bf16).reshape(
        depth, 3, per_block, HEAD_DIM, size
    )
    others = [exchange(own[:, :2], TEAM, step, team) for step in range(1, team)]
    cotangent, *others = lax.optimization_barrier((cotangent, *others))
    upstream_low = to_tokens(cotangent, depth) * token_mask.astype(bf16)
    attended, logs = attend(own, others, valid)
    attended_blocks = attended.reshape(depth, block_width, size)
    middle = resident + product("zde,zet->dt", output_full, attended_blocks)
    normed_two, inverse_two = normalize(middle)
    hidden_two = (normed_two * gains[1][:, None]).astype(bf16)
    pre_act = product("zdu,dt->zut", expand_full, hidden_two)
    activated, slope = gelu_parts(pre_act)
    activated, slope = activated.astype(bf16), slope.astype(bf16)
    block_output = to_features(
        (middle + product("zdu,zut->dt", reduce_full, activated)).astype(bf16), depth
    )

    upstream = upstream_low.astype(jnp.float32)
    reduce_part = product("dt,zut->zdu", upstream_low, activated, bf16)
    pre_grad = (
        product("zdu,dt->zut", reduce_full, upstream_low) * slope.astype(jnp.float32)
    ).astype(bf16)
    expand_part = product("dt,zut->zdu", hidden_two, pre_grad, bf16)
    normed_two_grad = product("zdu,zut->dt", expand_full, pre_grad)
    middle_grad, gain_two_part = normalize_back(normed_two_grad, normed_two, inverse_two, gains[1])
    middle_grad = middle_grad + upstream
    middle_grad_low = middle_grad.astype(bf16)
    output_part = outer(middle_grad_low, attended_blocks)
    attended_grad = product("zde,dt->zet", output_full, middle_grad_low, bf16).reshape(width, size)
    own_grad, other_grads = attend_back(own, others, attended, attended_grad, logs, valid)
    own_grad, block_output = lax.optimization_barrier((own_grad, block_output))
    pair_grad = own_grad[:, :2].astype(jnp.float32)
    for step in range(1, team):
        pair_grad = pair_grad + exchange(other_grads[step - 1], TEAM, step, team).astype(
            jnp.float32
        )
    stacked = jnp.concatenate([pair_grad.astype(bf16), own_grad[:, 2:]], axis=1).reshape(
        depth, 3 * block_width, size
    )
    project_part = outer(hidden_one, stacked)
    normed_one_grad = product("zdu,zut->dt", project_full, stacked)
    input_grad, gain_one_part = normalize_back(normed_one_grad, normed_one, inverse_one, gains[0])
    input_grad, gain_grads, weight_grads = scatter_every(
        (input_grad + middle_grad).astype(bf16),
        jnp.stack([gain_one_part, gain_two_part]),
        [reduce_part, expand_part, project_part, output_part],
        rows_of_weight,
        depth,
    )
    input_grad = input_grad.astype(jnp.float32)
    gain_one_grad, gain_two_grad = gain_grads[0], gain_grads[1]
    reduce_grad, expand_grad, project_grad, output_grad = weight_grads
    reduce_grad, output_grad = reduce_grad.T, output_grad.T
    project_grad = jnp.stack(
        [project_grad[:, at * block_width : (at + 1) * block_width] for at in (2, 0, 1)]
    )

    scale = 1.0 / math.sqrt(rows_local * lax.axis_size(ROW))
    pm, pw, pa = update(
        project_weight, project_moment, project_average, project_grad, RATE_PROJECT * scale
    )
    om, ow, oa = update(
        output_weight, output_moment, output_average, output_grad, RATE_OUTPUT * scale
    )
    em, ew, ea = update(
        expand_weight, expand_moment, expand_average, expand_grad, RATE_EXPAND * scale
    )
    rm, rw, ra = update(
        reduce_weight, reduce_moment, reduce_average, reduce_grad, RATE_REDUCE * scale
    )
    fm, fw, fa = update(gain_first, first_moment, first_average, gain_one_grad, RATE_GAIN * scale)
    sm, sw, sa = update(
        gain_second, second_moment, second_average, gain_two_grad, RATE_GAIN * scale
    )
    return (
        block_output,
        input_grad,
        project_grad,
        pm,
        pw,
        pa,
        pw.astype(bf16),
        output_grad,
        om,
        ow,
        oa,
        ow.astype(bf16),
        expand_grad,
        em,
        ew,
        ea,
        ew.astype(bf16),
        reduce_grad,
        rm,
        rw,
        ra,
        rw.astype(bf16),
        gain_one_grad,
        fm,
        fw,
        fa,
        gain_two_grad,
        sm,
        sw,
        sa,
    )


def solution(mesh):
    rows, columns = mesh.shape["row"], mesh.shape["col"]
    finer = Mesh(
        mesh.devices.reshape(rows // 2, 2, CLIPS_PER_COLUMN, columns // CLIPS_PER_COLUMN),
        ("pair", "core", "zhi", "zlo"),
    )
    plane = P(COL, ROW)
    weights = (P(None, ROW, COL), plane, P(ROW, COL), plane)
    placed = (plane, plane, P(ROW))
    for spec in weights:
        placed += (spec,) * 3
    placed += (P(COL),) * 6
    results = (plane, plane)
    for spec in weights:
        results += (spec,) * 5
    results += (P(COL),) * 8
    return jax.shard_map(
        on_device, mesh=finer, in_specs=placed, out_specs=results, check_vma=False
    )
```
